32 devices in a mesh: dp: 8 (over z, y), section: 4 (over x, core).
Axes of the slice: x: 2, y: 2, z: 4, core: 2. Of those that a mesh axis runs over, the one named last changes fastest.
Arguments:
- real_in: bfloat16 [64, 144, 512], P('dp'), may hold values from -48 to 48
- fake_in: bfloat16 [64, 144, 512], P('dp'), may hold values from -48 to 48
- kernel_first: bfloat16 [5, 512, 1024], P(None, None, 'section'), may hold values from -0.15625 to 0.15625
- kernel_second: bfloat16 [5, 1024, 1024], P(None, None, 'section'), may hold values from -0.125 to 0.125
Outputs:
- layer_loss: float32 [2], replicated
- grad_first: float32 [512, 5, 1024], P('dp', None, 'section')
- grad_second: float32 [1024, 5, 1024], P('dp', None, 'section')
The draws below stay inside these ranges and needn't reach their ends.
All inputs are finite; a program needn't handle non-finite values.
Results may differ from the reference program's by a relative error of at most 0.012.
The reference program's roundings to bfloat16 on the way count: a program that leaves them out, or rounds other values in their place, can miss the bound.
Values may be sent and summed in bfloat16 or wider, within the bound.
A program may use at most 128 MiB of HBM per device.

```python
import jax
import jax.numpy as jnp
from jax import lax

C = 1024
CIN = 512
K = 5
FRAMES = 48
COLS = 8
FRAMES_IN = 144
ROWS_ALL = 64


def draw_signal(key):
    subkeys = jax.random.split(key, 2)
    values_drawn = jnp.clip(jax.random.normal(subkeys[0], (ROWS_ALL, FRAMES_IN, CIN), jnp.float32), -4.0, 4.0)
    positions = jnp.arange(ROWS_ALL, dtype=jnp.float32)
    row_scale = 3.0 ** (positions / max(ROWS_ALL - 1, 1))
    channel_gain = jax.random.uniform(subkeys[1], (CIN,), jnp.float32, 0.5, 2.0)
    return (values_drawn * row_scale[:, None, None] * channel_gain).astype(jnp.bfloat16)


def draw_real_in(key, part):
    return draw_signal(jax.random.fold_in(key, 11))


def draw_fake_in(key, part):
    return draw_signal(jax.random.fold_in(key, 12))


def levels(own_key, dims, cuts, low, top_value):
    level, own = 1.0, jax.random.fold_in(own_key, 6)
    for axis_at, shards_of in cuts:
        draws = jnp.exp(jax.random.uniform(jax.random.fold_in(own, axis_at), (shards_of,), jnp.float32, low / len(cuts), top_value / len(cuts)))
        level = level * jnp.repeat(draws, dims[axis_at] // shards_of).reshape([-1 if axis == axis_at else 1 for axis in range(len(dims))])
    return level


def gaussian(own_key, dims, scale, reach, cuts=(), held_as=jnp.bfloat16):
    result = scale * jax.random.normal(own_key, dims, jnp.float32)
    if cuts:
        result = result * levels(own_key, dims, cuts, -0.22, 0.18)
    return jnp.clip(result, -reach, reach).astype(held_as)


def setup_inputs(seed: int = 0) -> dict:
    streams_of = jax.random.split(jax.random.key(seed), 5)
    real_in = draw_real_in(jax.random.fold_in(streams_of[4], 71), 0)
    fake_in = draw_fake_in(jax.random.fold_in(streams_of[4], 71), 0)
    kernel_first = gaussian(streams_of[2], (K, CIN, C), (K * CIN // 2) ** -0.5, 0.15625, ((2, 4),))
    kernel_second = gaussian(streams_of[3], (K, C, C), (K * C // 2) ** -0.5, 0.125, ((2, 4),))
    return dict(real_in=real_in, fake_in=fake_in, kernel_first=kernel_first, kernel_second=kernel_second)


smooth_width = 0.1
leak_slope = 0.1

def conv_strided(values, kernel, frames):
    padded = jnp.pad(values, ((0, 0), (2, 2), (0, 0)))
    summed = jnp.zeros((values.shape[0] * frames, kernel.shape[2]), jnp.float32)
    for tap in range(kernel.shape[0]):
        window = padded[:, tap:tap + 3 * frames - 2:3].reshape(-1, values.shape[2])
        summed = summed + jnp.dot(window, kernel[tap], preferred_element_type=jnp.float32)
    return summed.reshape(values.shape[0], frames, -1)

def conv_forward(values, kernel):
    frames = values.shape[1]
    padded = jnp.pad(values, ((0, 0), (2, 2), (0, 0)))
    summed = jnp.zeros((values.shape[0] * frames, kernel.shape[2]), jnp.float32)
    for tap in range(kernel.shape[0]):
        window = padded[:, tap:tap + frames].reshape(-1, values.shape[2])
        summed = summed + jnp.dot(window, kernel[tap], preferred_element_type=jnp.float32)
    return summed.reshape(values.shape[0], frames, -1)

def conv_backward(delta, kernel):
    frames = delta.shape[1]
    padded = jnp.pad(delta, ((0, 0), (2, 2), (0, 0)))
    summed = jnp.zeros((delta.shape[0] * frames, kernel.shape[1]), jnp.float32)
    for tap in range(kernel.shape[0]):
        window = padded[:, 4 - tap:4 - tap + frames].reshape(-1, delta.shape[2])
        summed = summed + lax.dot_general(window, kernel[tap], (((1,), (1,)), ((), ())), preferred_element_type=jnp.float32)
    return summed.reshape(delta.shape[0], frames, -1)

def weight_term(values, delta, offset, amount, stride):
    frames = delta.shape[1]
    padded = jnp.pad(values, ((0, 0), (2, 2), (0, 0)))
    padded = lax.dynamic_slice_in_dim(padded, offset, amount, 2)
    flat_delta = delta.reshape(-1, delta.shape[2])
    pieces = []
    for tap in range(K):
        window = padded[:, tap:tap + stride * (frames - 1) + 1:stride].reshape(-1, amount)
        pieces.append(lax.dot_general(window, flat_delta, (((0,), (0,)), ((), ())), preferred_element_type=jnp.float32))
    return jnp.stack(pieces, axis=1)

def activate(pre):
    return jnp.where(pre > 0, pre, leak_slope * pre).astype(jnp.bfloat16)

def local_grad(feature, normaliser):
    half = feature.shape[0] // 2
    difference = feature[:half].astype(jnp.float32) - feature[half:].astype(jnp.float32)
    slope = difference / jnp.sqrt(difference * difference + smooth_width * smooth_width) / normaliser
    return jnp.concatenate([slope, -slope], axis=0)

def smooth_total(feature):
    half = feature.shape[0] // 2
    difference = feature[:half].astype(jnp.float32) - feature[half:].astype(jnp.float32)
    return jnp.sum(jnp.sqrt(difference * difference + smooth_width * smooth_width) - smooth_width)

def reference(real_in, fake_in, kernel_first, kernel_second):
    row_total = real_in.shape[0]
    normaliser = float(COLS * FRAMES)
    values = jnp.concatenate([real_in, fake_in], axis=0)
    first = activate(conv_strided(values, kernel_first, FRAMES))
    second = activate(conv_forward(first, kernel_second))
    count_all = float(row_total * FRAMES * C)
    losses = jnp.stack([smooth_total(first) / count_all, smooth_total(second) / count_all])
    delta_second = (local_grad(second, normaliser) * jnp.where(second > 0, 1.0, leak_slope)).astype(jnp.bfloat16)
    grad_second = weight_term(first, delta_second, 0, C, 1)
    upstream = conv_backward(delta_second, kernel_second).astype(jnp.bfloat16).astype(jnp.float32)
    delta_first = ((local_grad(first, normaliser) + upstream) * jnp.where(first > 0, 1.0, leak_slope)).astype(jnp.bfloat16)
    grad_first = weight_term(values, delta_first, 0, CIN, 3)
    return (losses, grad_first, grad_second)
```

```python
import functools

import jax
import jax.numpy as jnp
from jax import lax
from jax.experimental import pallas as pl
from jax.experimental.pallas import tpu as pltpu
from jax.sharding import PartitionSpec as P

smooth_width = 0.1
leak_slope = 0.1
F32 = jnp.float32
BF16 = jnp.bfloat16
MESH = pl.DeviceIdType.MESH


def dot(a, b, ca=1, cb=0):
    return lax.dot_general(a, b, (((ca,), (cb,)), ((), ())), preferred_element_type=F32)


def leaky(pre):
    return jnp.where(pre > 0, pre, leak_slope * pre).astype(BF16)


def kernel(
    ndp, nsec, frames, normaliser,
    real, fake, w1h, w2h,
    loss_o, g1_o, g2_o,
    x, w1, w2, hall, acc, slopes, dk, us, ur, own_up, s2, s1, r2, r1, lsec, ldp,
    in_sem, hs, hr, uss, urs, g2s, g2r, g1s, g1r, lss, lsr, lds, ldr,
):
    dp, sec = lax.axis_index("dp"), lax.axis_index("section")
    rows, width = acc.shape
    half = rows // 2
    taps = w2.shape[0]
    cin = g1_o.shape[1] * ndp
    c2, c1 = g2_o.shape[1], g1_o.shape[1]

    def sec_at(j):
        return lax.rem(sec + j, nsec)

    def dp_at(j):
        return lax.rem(dp + j, ndp)

    loads = [
        pltpu.make_async_copy(real, x.at[pl.ds(0, half)], in_sem.at[0]),
        pltpu.make_async_copy(fake, x.at[pl.ds(half, half)], in_sem.at[1]),
        pltpu.make_async_copy(w1h, w1, in_sem.at[2]),
        pltpu.make_async_copy(w2h, w2, in_sem.at[3]),
    ]
    for c in loads:
        c.start()

    barrier = pltpu.get_barrier_semaphore()
    for j in range(1, nsec):
        pl.semaphore_signal(barrier, inc=1, device_id={"section": sec_at(j)}, device_id_type=MESH)
    for j in range(1, ndp):
        pl.semaphore_signal(barrier, inc=1, device_id={"dp": dp_at(j)}, device_id_type=MESH)

    time = lax.rem(lax.broadcasted_iota(jnp.int32, (rows, width), 0), frames)

    def shift(p, s):
        if s == 0:
            return p
        rolled = pltpu.roll(p, (-s) % rows, 0)
        keep = (time + s >= 0) & (time + s < frames)
        return jnp.where(keep, rolled, 0.0)

    def remote(src, dst, ss, rs, **to):
        c = pltpu.make_async_remote_copy(
            src_ref=src, dst_ref=dst, send_sem=ss, recv_sem=rs, device_id=to, device_id_type=MESH
        )
        c.start()
        return c

    for c in loads[:3]:
        c.wait()
    early = dot(x[:, pl.ds(cin, 2 * cin)], w1[pl.ds(0, 2 * cin), :])
    pre1 = dot(x[...], w1[pl.ds(2 * cin, 3 * cin), :]) + shift(early, -1)
    hall[0] = leaky(pre1)

    pl.semaphore_wait(barrier, nsec - 1 + ndp - 1)
    h_copies = [
        remote(hall.at[0], hall.at[j], hs.at[j - 1], hr.at[j - 1], section=sec_at(j))
        for j in range(1, nsec)
    ]

    def smooth(feature):
        h = feature.astype(F32)
        d = h[:half] - h[half:]
        s = d * d + smooth_width * smooth_width
        inv = lax.rsqrt(s)
        total = jnp.sum(s * inv - smooth_width, axis=0, keepdims=True)
        total = jnp.sum(total, axis=1, keepdims=True)
        q = d * inv * (1.0 / normaliser)
        gate = jnp.where(h > 0, 1.0, leak_slope)
        return total, q, gate

    total1, q1, gate1 = smooth(hall[0])
    slopes[pl.ds(0, half), :] = q1
    slopes[pl.ds(half, half), :] = -q1

    loads[3].wait()
    for j in range(nsec):
        if j:
            h_copies[j - 1].wait_recv()
        owner = lax.rem(sec - j + nsec, nsec)
        block = hall[j]
        part = None
        for k in range(taps):
            p = shift(dot(block, w2[k, pl.ds(pl.multiple_of(owner * width, width), width), :]), k - 2)
            part = p if part is None else part + p
        acc[...] = part if j == 0 else acc[...] + part
    h2 = leaky(acc[...])
    total2, q2, gate2 = smooth(h2)
    line = lax.broadcasted_iota(jnp.int32, lsec.shape[1:], 0)
    lsec[0] = jnp.where(line == 0, total1, jnp.where(line == 1, total2, 0.0))
    l_copies = [
        remote(lsec.at[0], lsec.at[j], lss.at[j - 1], lsr.at[j - 1], section=sec_at(j))
        for j in range(1, nsec)
    ]
    delta2 = jnp.concatenate([q2, -q2], axis=0) * gate2
    for k in range(taps):
        dk[k] = shift(delta2, 2 - k).astype(BF16)

    u_copies = []
    for j in list(range(1, nsec)) + [0]:
        at = pl.multiple_of(sec_at(j) * width, width)
        up = None
        for k in range(taps):
            p = dot(dk[k], w2[k, pl.ds(at, width), :], 1, 1)
            up = p if up is None else up + p
        if j:
            us[j - 1] = up.astype(BF16)
            u_copies.append(
                remote(us.at[j - 1], ur.at[j - 1], uss.at[j - 1], urs.at[j - 1], section=sec_at(j))
            )
        else:
            own_up[...] = up

    for j in range(nsec):
        owner = lax.rem(sec - j + nsec, nsec)
        at = pl.multiple_of(owner * width, width)
        block = hall[j]
        for k in range(taps):
            s2[k, pl.ds(at, width), :] = dot(block, dk[k], 0, 0).astype(BF16)
    g2_copies = []
    for j in range(1, ndp):
        at = pl.multiple_of(dp_at(j) * c2, c2)
        g2_copies.append(
            remote(s2.at[:, pl.ds(at, c2), :], r2.at[j - 1], g2s.at[j - 1], g2r.at[j - 1], dp=dp_at(j))
        )

    up = own_up[...]
    for j in range(1, nsec):
        u_copies[j - 1].wait_recv()
        up = up + ur[j - 1].astype(F32)
    h1 = hall[0].astype(F32)
    delta1 = (slopes[...] + up.astype(BF16).astype(F32)) * jnp.where(h1 > 0, 1.0, leak_slope)
    ahead = shift(delta1, 1).astype(BF16)
    delta1 = delta1.astype(BF16)
    for k in range(taps):
        phase = (k + 1) % 3
        s1[k] = dot(x[:, pl.ds(phase * cin, cin)], ahead if k < 2 else delta1, 0, 0).astype(BF16)
    g1_copies = []
    for j in range(1, ndp):
        at = pl.multiple_of(dp_at(j) * c1, c1)
        g1_copies.append(
            remote(s1.at[:, pl.ds(at, c1), :], r1.at[j - 1], g1s.at[j - 1], g1r.at[j - 1], dp=dp_at(j))
        )

    for c in l_copies:
        c.wait()
    ldp[0] = functools.reduce(
        lambda a, b: a + b, [lsec[lax.rem(sec - g + nsec, nsec)] for g in range(nsec)]
    )
    ld_copies = [
        remote(ldp.at[0], ldp.at[j], lds.at[j - 1], ldr.at[j - 1], dp=dp_at(j)) for j in range(1, ndp)
    ]

    for k in range(taps):
        g2_o[k] = s2[k, pl.ds(pl.multiple_of(dp * c2, c2), c2), :].astype(F32)
        g1_o[k] = s1[k, pl.ds(pl.multiple_of(dp * c1, c1), c1), :].astype(F32)
    for j in range(1, ndp):
        g2_copies[j - 1].wait_recv()
        g2_o[...] += r2[j - 1].astype(F32)
    for j in range(1, ndp):
        g1_copies[j - 1].wait_recv()
        g1_o[...] += r1[j - 1].astype(F32)
    for c in ld_copies:
        c.wait()
    loss_o[...] = functools.reduce(
        lambda a, b: a + b, [ldp[lax.rem(dp - g + ndp, ndp)] for g in range(ndp)]
    )
    for c in h_copies + u_copies + g2_copies + g1_copies:
        c.wait_send()


def shards(ndp, nsec, real_in, fake_in, kernel_first, kernel_second):
    cols, frames_in, cin = real_in.shape
    frames = frames_in // 3
    taps, whole, width = kernel_second.shape
    normaliser = float(cols * frames)
    count_all = float(cols * ndp * frames * whole)
    half = cols * frames
    rows = 2 * half
    c1, c2 = cin // ndp, whole // ndp
    dma = pltpu.SemaphoreType.DMA
    loss, g1, g2 = pl.pallas_call(
        functools.partial(kernel, ndp, nsec, frames, normaliser),
        out_shape=(
            jax.ShapeDtypeStruct((8, 128), F32),
            jax.ShapeDtypeStruct((taps, c1, width), F32),
            jax.ShapeDtypeStruct((taps, c2, width), F32),
        ),
        in_specs=[pl.BlockSpec(memory_space=pl.ANY)] * 4,
        out_specs=(pl.BlockSpec(memory_space=pltpu.VMEM),) * 3,
        scratch_shapes=[
            pltpu.VMEM((rows, 3 * cin), BF16),
            pltpu.VMEM((taps * cin, width), BF16),
            pltpu.VMEM((taps, whole, width), BF16),
            pltpu.VMEM((nsec, rows, width), BF16),
            pltpu.VMEM((rows, width), F32),
            pltpu.VMEM((rows, width), F32),
            pltpu.VMEM((taps, rows, width), BF16),
            pltpu.VMEM((nsec - 1, rows, width), BF16),
            pltpu.VMEM((nsec - 1, rows, width), BF16),
            pltpu.VMEM((rows, width), F32),
            pltpu.VMEM((taps, whole, width), BF16),
            pltpu.VMEM((taps, cin, width), BF16),
            pltpu.VMEM((ndp - 1, taps, c2, width), BF16),
            pltpu.VMEM((ndp - 1, taps, c1, width), BF16),
            pltpu.VMEM((nsec, 8, 128), F32),
            pltpu.VMEM((ndp, 8, 128), F32),
            dma((4,)),
            dma((nsec - 1,)), dma((nsec - 1,)),
            dma((nsec - 1,)), dma((nsec - 1,)),
            dma((ndp - 1,)), dma((ndp - 1,)),
            dma((ndp - 1,)), dma((ndp - 1,)),
            dma((nsec - 1,)), dma((nsec - 1,)),
            dma((ndp - 1,)), dma((ndp - 1,)),
        ],
        compiler_params=pltpu.CompilerParams(collective_id=0, has_side_effects=True),
    )(
        real_in.reshape(half, 3 * cin),
        fake_in.reshape(half, 3 * cin),
        kernel_first.reshape(taps * cin, width),
        kernel_second,
    )
    return loss[:2, 0] / count_all, g1.transpose(1, 0, 2), g2.transpose(1, 0, 2)


def solution(mesh):
    return jax.shard_map(
        functools.partial(shards, mesh.shape["dp"], mesh.shape["section"]),
        mesh=mesh,
        in_specs=(
            P("dp", None, None),
            P("dp", None, None),
            P(None, None, "section"),
            P(None, None, "section"),
        ),
        out_specs=(P(), P("dp", None, "section"), P("dp", None, "section")),
        check_vma=False,
    )
```

```python
import functools

import jax
import jax.numpy as jnp
from jax import lax
from jax.experimental import pallas as pl
from jax.experimental.pallas import tpu as pltpu
from jax.sharding import PartitionSpec as P

smooth_width = 0.1
leak_slope = 0.1
F32 = jnp.float32
BF16 = jnp.bfloat16
MESH = pl.DeviceIdType.MESH


def dot(a, b, ca=1, cb=0):
    return lax.dot_general(a, b, (((ca,), (cb,)), ((), ())), preferred_element_type=F32)


def leaky(pre):
    return jnp.where(pre > 0, pre, leak_slope * pre).astype(BF16)


def kernel(
    ndp, nsec, frames, normaliser,
    real, fake, w1h, w2h,
    loss_o, g1_o, g2_o,
    x, w1, w2, hall, acc, slopes, dk, us, ur, own_up, s2, s1, y2, y1, z2, z1, r2, r1, lsec, ldp,
    in_sem, hs, hr, uss, urs, y2s, y2r, y1s, y1r, z2s, z2r, z1s, z1r, lss, lsr, lds, ldr,
):
    dp, sec = lax.axis_index("dp"), lax.axis_index("section")
    rows, width = acc.shape
    half = rows // 2
    taps = w2.shape[0]
    cin = g1_o.shape[1] * ndp
    c2, c1 = g2_o.shape[1], g1_o.shape[1]

    inner, outer = lax.rem(dp, 2), dp // 2
    nout = ndp // 2
    span = nout // nsec
    group, place = outer // span, lax.rem(outer, span)
    partner = dp + 1 - 2 * inner
    sec_inner, sec_outer = lax.rem(sec, 2), sec // 2
    sec_outers = nsec // 2
    sec_partner = sec + 1 - 2 * sec_inner

    def owner_of(slot):
        jo, ji = slot // 2, slot % 2
        return lax.rem(sec_outer - jo + sec_outers, sec_outers) * 2 + lax.rem(sec_inner + ji, 2)

    def outer_at(jb, i):
        return lax.rem(group + jb, nsec) * span + lax.rem(place + i, span)

    def sec_at(j):
        return lax.rem(sec + j, nsec)

    def dp_at(j):
        return lax.rem(dp + j, ndp)

    loads = [
        pltpu.make_async_copy(real, x.at[pl.ds(0, half)], in_sem.at[0]),
        pltpu.make_async_copy(fake, x.at[pl.ds(half, half)], in_sem.at[1]),
        pltpu.make_async_copy(w1h, w1, in_sem.at[2]),
        pltpu.make_async_copy(w2h, w2, in_sem.at[3]),
    ]
    for c in loads:
        c.start()

    barrier = pltpu.get_barrier_semaphore()
    for j in range(1, nsec):
        pl.semaphore_signal(barrier, inc=1, device_id={"section": sec_at(j)}, device_id_type=MESH)
    for j in range(1, ndp):
        pl.semaphore_signal(barrier, inc=1, device_id={"dp": dp_at(j)}, device_id_type=MESH)

    time = lax.rem(lax.broadcasted_iota(jnp.int32, (rows, width), 0), frames)

    def shift(p, s):
        if s == 0:
            return p
        rolled = pltpu.roll(p, (-s) % rows, 0)
        keep = (time + s >= 0) & (time + s < frames)
        return jnp.where(keep, rolled, 0.0)

    def remote(src, dst, ss, rs, **to):
        c = pltpu.make_async_remote_copy(
            src_ref=src, dst_ref=dst, send_sem=ss, recv_sem=rs, device_id=to, device_id_type=MESH
        )
        c.start()
        return c

    for c in loads[:3]:
        c.wait()
    early = dot(x[:, pl.ds(cin, 2 * cin)], w1[pl.ds(0, 2 * cin), :])
    pre1 = dot(x[...], w1[pl.ds(2 * cin, 3 * cin), :]) + shift(early, -1)
    hall[0] = leaky(pre1)

    pl.semaphore_wait(barrier, nsec - 1 + ndp - 1)
    halves = [pl.ds(0, half), pl.ds(half, half)]
    h_direct, h_passed = {}, {}
    for c, at in enumerate(halves):
        for jo in range(1, sec_outers):
            to = lax.rem(sec_outer + jo, sec_outers) * 2 + sec_inner
            h_direct[2 * jo, c] = remote(
                hall.at[0, at], hall.at[2 * jo, at], hs.at[2 * jo, c], hr.at[2 * jo, c], section=to
            )
    for c, at in enumerate(halves):
        h_direct[1, c] = remote(
            hall.at[0, at], hall.at[1, at], hs.at[1, c], hr.at[1, c], section=sec_partner
        )

    def smooth(feature):
        h = feature.astype(F32)
        d = h[:half] - h[half:]
        s = d * d + smooth_width * smooth_width
        inv = lax.rsqrt(s)
        total = jnp.sum(s * inv - smooth_width, axis=0, keepdims=True)
        total = jnp.sum(total, axis=1, keepdims=True)
        q = d * inv * (1.0 / normaliser)
        gate = jnp.where(h > 0, 1.0, leak_slope)
        return total, q, gate

    total1, q1, gate1 = smooth(hall[0])
    slopes[pl.ds(0, half), :] = q1
    slopes[pl.ds(half, half), :] = -q1

    loads[3].wait()
    for j in range(nsec):
        if j == 2:
            for c, at in enumerate(halves):
                for jo in range(1, sec_outers):
                    h_direct[2 * jo, c].wait_recv()
                    h_passed[2 * jo + 1, c] = remote(
                        hall.at[2 * jo, at],
                        hall.at[2 * jo + 1, at],
                        hs.at[2 * jo + 1, c],
                        hr.at[2 * jo + 1, c],
                        section=sec_partner,
                    )
        if j % 2:
            for c in range(2):
                (h_direct if j == 1 else h_passed)[j, c].wait_recv()
        owner = owner_of(j)
        block = hall[j]
        part = None
        for k in range(taps):
            p = shift(dot(block, w2[k, pl.ds(pl.multiple_of(owner * width, width), width), :]), k - 2)
            part = p if part is None else part + p
        acc[...] = part if j == 0 else acc[...] + part
    h2 = leaky(acc[...])
    total2, q2, gate2 = smooth(h2)
    line = lax.broadcasted_iota(jnp.int32, lsec.shape[1:], 0)
    lsec[0] = jnp.where(line == 0, total1, jnp.where(line == 1, total2, 0.0))
    l_copies = [
        remote(lsec.at[0], lsec.at[j], lss.at[j - 1], lsr.at[j - 1], section=sec_at(j))
        for j in range(1, nsec)
    ]
    delta2 = jnp.concatenate([q2, -q2], axis=0) * gate2
    for k in range(taps):
        dk[k] = shift(delta2, 2 - k).astype(BF16)

    order = [(jb, i) for jb in range(1, nsec) for i in range(span)] + [(0, i) for i in range(1, span)] + [(0, 0)]

    def exchange(send, land, ss, rs, rows_of, group_at):
        copies = []
        for n, (jb, i) in enumerate(order):
            if jb != group_at:
                continue
            at = pl.multiple_of((outer_at(jb, i) * 2 + 1 - inner) * rows_of, rows_of)
            copies.append(
                remote(send.at[:, pl.ds(at, rows_of), :], land.at[n], ss.at[n], rs.at[n], dp=partner)
            )
        return copies

    def relay(copy, n, send, land, out, pair, final, ss, rs, rows_of):
        jb, i = order[n]
        to = outer_at(jb, i)
        at = pl.multiple_of((to * 2 + inner) * rows_of, rows_of)
        copy.wait_recv()
        both = send[:, pl.ds(at, rows_of), :].astype(F32) + land[n].astype(F32)
        if n == nout - 1:
            out[...] = both
            return None
        pair[n] = both.astype(BF16)
        return remote(pair.at[n], final.at[n], ss.at[n], rs.at[n], dp=to * 2 + inner)

    y2c, z2c, y1c, z1c = [], [], [], []
    for jb in list(range(1, nsec)) + [0]:
        owner = lax.rem(group + jb, nsec)
        slot = lax.rem(sec_outer - owner // 2 + sec_outers, sec_outers) * 2 + lax.rem(
            sec_inner + lax.rem(owner, 2), 2
        )
        at = pl.multiple_of(owner * width, width)
        block = hall[slot]
        for k in range(taps):
            s2[k, pl.ds(at, width), :] = dot(block, dk[k], 0, 0).astype(BF16)
        y2c += exchange(s2, y2, y2s, y2r, c2, jb)

    u_copies = []
    for j in list(range(1, nsec)) + [0]:
        at = pl.multiple_of(sec_at(j) * width, width)
        up = None
        for k in range(taps):
            p = dot(dk[k], w2[k, pl.ds(at, width), :], 1, 1)
            up = p if up is None else up + p
        if j:
            us[j - 1] = up.astype(BF16)
            u_copies.append(
                remote(us.at[j - 1], ur.at[j - 1], uss.at[j - 1], urs.at[j - 1], section=sec_at(j))
            )
        else:
            own_up[...] = up

    for c in l_copies:
        c.wait()
    ldp[0] = functools.reduce(
        lambda a, b: a + b, [lsec[lax.rem(sec - g + nsec, nsec)] for g in range(nsec)]
    )
    ld_copies = [
        remote(ldp.at[0], ldp.at[j], lds.at[j - 1], ldr.at[j - 1], dp=dp_at(j)) for j in range(1, ndp)
    ]

    for n in range(nout - 1):
        z2c.append(relay(y2c[n], n, s2, y2, g2_o, z2, r2, z2s, z2r, c2))

    up = own_up[...]
    for j in range(1, nsec):
        u_copies[j - 1].wait_recv()
        up = up + ur[j - 1].astype(F32)
    h1 = hall[0].astype(F32)
    delta1 = (slopes[...] + up.astype(BF16).astype(F32)) * jnp.where(h1 > 0, 1.0, leak_slope)
    ahead = shift(delta1, 1).astype(BF16)
    delta1 = delta1.astype(BF16)
    for k in range(taps):
        phase = (k + 1) % 3
        s1[k] = dot(x[:, pl.ds(phase * cin, cin)], ahead if k < 2 else delta1, 0, 0).astype(BF16)
    for jb in list(range(1, nsec)) + [0]:
        y1c += exchange(s1, y1, y1s, y1r, c1, jb)

    relay(y2c[-1], nout - 1, s2, y2, g2_o, z2, r2, z2s, z2r, c2)
    for n in range(nout - 1):
        z2c[n].wait_recv()
        g2_o[...] += r2[n].astype(F32)
    for n in range(nout):
        z1c.append(relay(y1c[n], n, s1, y1, g1_o, z1, r1, z1s, z1r, c1))
    z1c = z1c[:-1]
    for c in ld_copies:
        c.wait()
    loss_o[...] = functools.reduce(
        lambda a, b: a + b, [ldp[lax.rem(dp - g + ndp, ndp)] for g in range(ndp)]
    )
    for n in range(nout - 1):
        z1c[n].wait_recv()
        g1_o[...] += r1[n].astype(F32)
    for c in list(h_direct.values()) + list(h_passed.values()) + u_copies + y2c + z2c + y1c + z1c:
        c.wait_send()


def shards(ndp, nsec, real_in, fake_in, kernel_first, kernel_second):
    cols, frames_in, cin = real_in.shape
    frames = frames_in // 3
    taps, whole, width = kernel_second.shape
    normaliser = float(cols * frames)
    count_all = float(cols * ndp * frames * whole)
    half = cols * frames
    rows = 2 * half
    c1, c2 = cin // ndp, whole // ndp
    nout = ndp // 2
    dma = pltpu.SemaphoreType.DMA
    loss, g1, g2 = pl.pallas_call(
        functools.partial(kernel, ndp, nsec, frames, normaliser),
        out_shape=(
            jax.ShapeDtypeStruct((8, 128), F32),
            jax.ShapeDtypeStruct((taps, c1, width), F32),
            jax.ShapeDtypeStruct((taps, c2, width), F32),
        ),
        in_specs=[pl.BlockSpec(memory_space=pl.ANY)] * 4,
        out_specs=(pl.BlockSpec(memory_space=pltpu.VMEM),) * 3,
        scratch_shapes=[
            pltpu.VMEM((rows, 3 * cin), BF16),
            pltpu.VMEM((taps * cin, width), BF16),
            pltpu.VMEM((taps, whole, width), BF16),
            pltpu.VMEM((nsec, rows, width), BF16),
            pltpu.VMEM((rows, width), F32),
            pltpu.VMEM((rows, width), F32),
            pltpu.VMEM((taps, rows, width), BF16),
            pltpu.VMEM((nsec - 1, rows, width), BF16),
            pltpu.VMEM((nsec - 1, rows, width), BF16),
            pltpu.VMEM((rows, width), F32),
            pltpu.VMEM((taps, whole, width), BF16),
            pltpu.VMEM((taps, cin, width), BF16),
            pltpu.VMEM((nout, taps, c2, width), BF16),
            pltpu.VMEM((nout, taps, c1, width), BF16),
            pltpu.VMEM((nout, taps, c2, width), BF16),
            pltpu.VMEM((nout, taps, c1, width), BF16),
            pltpu.VMEM((nout, taps, c2, width), BF16),
            pltpu.VMEM((nout, taps, c1, width), BF16),
            pltpu.VMEM((nsec, 8, 128), F32),
            pltpu.VMEM((ndp, 8, 128), F32),
            dma((4,)),
            dma((nsec, 2)), dma((nsec, 2)),
            dma((nsec - 1,)), dma((nsec - 1,)),
            dma((nout,)), dma((nout,)), dma((nout,)), dma((nout,)),
            dma((nout,)), dma((nout,)), dma((nout,)), dma((nout,)),
            dma((nsec - 1,)), dma((nsec - 1,)),
            dma((ndp - 1,)), dma((ndp - 1,)),
        ],
        compiler_params=pltpu.CompilerParams(collective_id=0, has_side_effects=True),
    )(
        real_in.reshape(half, 3 * cin),
        fake_in.reshape(half, 3 * cin),
        kernel_first.reshape(taps * cin, width),
        kernel_second,
    )
    return loss[:2, 0] / count_all, g1.transpose(1, 0, 2), g2.transpose(1, 0, 2)


def solution(mesh):
    return jax.shard_map(
        functools.partial(shards, mesh.shape["dp"], mesh.shape["section"]),
        mesh=mesh,
        in_specs=(
            P("dp", None, None),
            P("dp", None, None),
            P(None, None, "section"),
            P(None, None, "section"),
        ),
        out_specs=(P(), P("dp", None, "section"), P("dp", None, "section")),
        check_vma=False,
    )
```

```python
import functools

import jax
import jax.numpy as jnp
from jax import lax
from jax.experimental import pallas as pl
from jax.experimental.pallas import tpu as pltpu
from jax.sharding import PartitionSpec as P

smooth_width = 0.1
leak_slope = 0.1
F32 = jnp.float32
BF16 = jnp.bfloat16
MESH = pl.DeviceIdType.MESH


def dot(a, b, ca=1, cb=0):
    return lax.dot_general(a, b, (((ca,), (cb,)), ((), ())), preferred_element_type=F32)


def leaky(pre):
    return jnp.where(pre > 0, pre, leak_slope * pre).astype(BF16)


def kernel(
    ndp, nsec, frames, normaliser,
    real, fake, w1h, w2h,
    loss_o, g1_o, g2_o,
    raw, wide, x, w1, w2, hall, acc, slopes, dk, us, ur, own_up, s2, s1, y2, y1, z2, z1, r2, r1, lsec, ldp,
    in_sem, hs, hr, uss, urs, y2s, y2r, y1s, y1r, z2s, z2r, z1s, z1r, lss, lsr, lds, ldr,
):
    dp, sec = lax.axis_index("dp"), lax.axis_index("section")
    rows, width = acc.shape
    half = rows // 2
    taps = w2.shape[0]
    cin = g1_o.shape[1] * ndp
    c2, c1 = g2_o.shape[1], g1_o.shape[1]

    inner, outer = lax.rem(dp, 2), dp // 2
    nout = ndp // 2
    span = nout // nsec
    group, place = outer // span, lax.rem(outer, span)
    partner = dp + 1 - 2 * inner
    sec_inner, sec_outer = lax.rem(sec, 2), sec // 2
    sec_outers = nsec // 2
    sec_partner = sec + 1 - 2 * sec_inner

    def owner_of(slot):
        jo, ji = slot // 2, slot % 2
        return lax.rem(sec_outer - jo + sec_outers, sec_outers) * 2 + lax.rem(sec_inner + ji, 2)

    def outer_at(jb, i):
        return lax.rem(group + jb, nsec) * span + lax.rem(place + i, span)

    def sec_at(j):
        return lax.rem(sec + j, nsec)

    def dp_at(j):
        return lax.rem(dp + j, ndp)

    loads = [
        pltpu.make_async_copy(real, raw.at[0], in_sem.at[0]),
        pltpu.make_async_copy(w1h, w1, in_sem.at[2]),
        pltpu.make_async_copy(fake, raw.at[1], in_sem.at[1]),
        pltpu.make_async_copy(w2h, w2, in_sem.at[3]),
    ]
    for c in loads:
        c.start()

    barrier = pltpu.get_barrier_semaphore()
    for j in range(1, nsec):
        pl.semaphore_signal(barrier, inc=1, device_id={"section": sec_at(j)}, device_id_type=MESH)
    for j in range(1, ndp):
        pl.semaphore_signal(barrier, inc=1, device_id={"dp": dp_at(j)}, device_id_type=MESH)

    time = lax.rem(lax.broadcasted_iota(jnp.int32, (rows, width), 0), frames)

    def shift(p, s):
        if s == 0:
            return p
        rolled = pltpu.roll(p, (-s) % p.shape[0], 0)
        at = time[: p.shape[0]]
        keep = (at + s >= 0) & (at + s < frames)
        return jnp.where(keep, rolled, 0.0)

    def remote(src, dst, ss, rs, **to):
        c = pltpu.make_async_remote_copy(
            src_ref=src, dst_ref=dst, send_sem=ss, recv_sem=rs, device_id=to, device_id_type=MESH
        )
        c.start()
        return c

    halves = [pl.ds(0, half), pl.ds(half, half)]
    h_direct, h_passed = {}, {}
    for c, at in enumerate(halves):
        loads[2 * c].wait()
        for b in range(cin // 128):
            wide[c * (cin // 128) + b] = raw[c, :, pl.ds(b * 128, 128)].astype(F32)
            for phase in range(3):
                lanes = wide[c * (cin // 128) + b, pl.ds(phase, half, stride=3), :]
                x[at, pl.ds(phase * cin + b * 128, 128)] = lanes.astype(BF16)
        if c == 0:
            loads[1].wait()
        early = dot(x[at, pl.ds(cin, 2 * cin)], w1[pl.ds(0, 2 * cin), :])
        pre1 = dot(x[at, :], w1[pl.ds(2 * cin, 3 * cin), :]) + shift(early, -1)
        hall[0, at] = leaky(pre1)
        if c == 0:
            pl.semaphore_wait(barrier, nsec - 1 + ndp - 1)
        for jo in range(1, sec_outers):
            to = lax.rem(sec_outer + jo, sec_outers) * 2 + sec_inner
            h_direct[2 * jo, c] = remote(
                hall.at[0, at], hall.at[2 * jo, at], hs.at[2 * jo, c], hr.at[2 * jo, c], section=to
            )
        h_direct[1, c] = remote(
            hall.at[0, at], hall.at[1, at], hs.at[1, c], hr.at[1, c], section=sec_partner
        )

    def smooth(feature):
        h = feature.astype(F32)
        d = h[:half] - h[half:]
        s = d * d + smooth_width * smooth_width
        inv = lax.rsqrt(s)
        total = jnp.sum(s * inv - smooth_width, axis=0, keepdims=True)
        total = jnp.sum(total, axis=1, keepdims=True)
        q = d * inv * (1.0 / normaliser)
        gate = jnp.where(h > 0, 1.0, leak_slope)
        return total, q, gate

    total1, q1, gate1 = smooth(hall[0])
    slopes[pl.ds(0, half), :] = q1
    slopes[pl.ds(half, half), :] = -q1

    loads[3].wait()
    for j in range(nsec):
        if j == 2:
            for c, at in enumerate(halves):
                for jo in range(1, sec_outers):
                    h_direct[2 * jo, c].wait_recv()
                    h_passed[2 * jo + 1, c] = remote(
                        hall.at[2 * jo, at],
                        hall.at[2 * jo + 1, at],
                        hs.at[2 * jo + 1, c],
                        hr.at[2 * jo + 1, c],
                        section=sec_partner,
                    )
        if j % 2:
            for c in range(2):
                (h_direct if j == 1 else h_passed)[j, c].wait_recv()
        owner = owner_of(j)
        block = hall[j]
        part = None
        for k in range(taps):
            p = shift(dot(block, w2[k, pl.ds(pl.multiple_of(owner * width, width), width), :]), k - 2)
            part = p if part is None else part + p
        acc[...] = part if j == 0 else acc[...] + part
    h2 = leaky(acc[...])
    total2, q2, gate2 = smooth(h2)
    line = lax.broadcasted_iota(jnp.int32, lsec.shape[1:], 0)
    lsec[0] = jnp.where(line == 0, total1, jnp.where(line == 1, total2, 0.0))
    l_copies = [
        remote(lsec.at[0], lsec.at[j], lss.at[j - 1], lsr.at[j - 1], section=sec_at(j))
        for j in range(1, nsec)
    ]
    delta2 = jnp.concatenate([q2, -q2], axis=0) * gate2
    for k in range(taps):
        dk[k] = shift(delta2, 2 - k).astype(BF16)

    order = [(jb, i) for jb in range(1, nsec) for i in range(span)] + [(0, i) for i in range(1, span)] + [(0, 0)]

    pieces = [pl.ds(0, taps // 2), pl.ds(taps // 2, taps - taps // 2)]

    def exchange(copies, send, land, ss, rs, rows_of, group_at, piece):
        cut = pieces[piece]
        for n, (jb, i) in enumerate(order):
            if jb != group_at:
                continue
            at = pl.multiple_of((outer_at(jb, i) * 2 + 1 - inner) * rows_of, rows_of)
            copies[n, piece] = remote(
                send.at[cut, pl.ds(at, rows_of), :],
                land.at[n, cut],
                ss.at[n, piece],
                rs.at[n, piece],
                dp=partner,
            )

    def relay(copies, n, piece, send, land, out, pair, final, ss, rs, rows_of):
        cut = pieces[piece]
        jb, i = order[n]
        to = outer_at(jb, i)
        at = pl.multiple_of((to * 2 + inner) * rows_of, rows_of)
        copies[n, piece].wait_recv()
        both = send[cut, pl.ds(at, rows_of), :].astype(F32) + land[n, cut].astype(F32)
        if n == nout - 1:
            out[cut] = both
            return []
        pair[n, cut] = both.astype(BF16)
        return [
            remote(
                pair.at[n, cut],
                final.at[n, cut],
                ss.at[n, piece],
                rs.at[n, piece],
                dp=to * 2 + inner,
            )
        ]

    def relay2(n, piece):
        return relay(y2c, n, piece, s2, y2, g2_o, z2, r2, z2s, z2r, c2)

    def relay1(n, piece):
        return relay(y1c, n, piece, s1, y1, g1_o, z1, r1, z1s, z1r, c1)

    y2c, z2c, y1c, z1c = {}, [], {}, []
    for jb in list(range(1, nsec)) + [0]:
        owner = lax.rem(group + jb, nsec)
        slot = lax.rem(sec_outer - owner // 2 + sec_outers, sec_outers) * 2 + lax.rem(
            sec_inner + lax.rem(owner, 2), 2
        )
        at = pl.multiple_of(owner * width, width)
        block = hall[slot]
        for piece, cut in enumerate(pieces):
            for k in range(cut.start, cut.start + cut.size):
                s2[k, pl.ds(at, width), :] = dot(block, dk[k], 0, 0).astype(BF16)
            exchange(y2c, s2, y2, y2s, y2r, c2, jb, piece)

    u_copies = []
    for j in list(range(1, nsec)) + [0]:
        at = pl.multiple_of(sec_at(j) * width, width)
        up = None
        for k in range(taps):
            p = dot(dk[k], w2[k, pl.ds(at, width), :], 1, 1)
            up = p if up is None else up + p
        if j:
            us[j - 1] = up.astype(BF16)
            u_copies.append(
                remote(us.at[j - 1], ur.at[j - 1], uss.at[j - 1], urs.at[j - 1], section=sec_at(j))
            )
        else:
            own_up[...] = up

    for c in l_copies:
        c.wait()
    ldp[0] = functools.reduce(
        lambda a, b: a + b, [lsec[lax.rem(sec - g + nsec, nsec)] for g in range(nsec)]
    )
    ld_copies = [
        remote(ldp.at[0], ldp.at[j], lds.at[j - 1], ldr.at[j - 1], dp=dp_at(j)) for j in range(1, ndp)
    ]

    for n in range(nout - 1):
        z2c += relay2(n, 0) + relay2(n, 1)

    up = own_up[...]
    for j in range(1, nsec):
        u_copies[j - 1].wait_recv()
        up = up + ur[j - 1].astype(F32)
    h1 = hall[0].astype(F32)
    delta1 = (slopes[...] + up.astype(BF16).astype(F32)) * jnp.where(h1 > 0, 1.0, leak_slope)
    ahead = shift(delta1, 1).astype(BF16)
    delta1 = delta1.astype(BF16)
    for piece, cut in enumerate(pieces):
        for k in range(cut.start, cut.start + cut.size):
            phase = (k + 1) % 3
            s1[k] = dot(x[:, pl.ds(phase * cin, cin)], ahead if k < 2 else delta1, 0, 0).astype(BF16)
    for jb in list(range(1, nsec)) + [0]:
        for piece in range(2):
            exchange(y1c, s1, y1, y1s, y1r, c1, jb, piece)

    relay2(nout - 1, 0)
    relay2(nout - 1, 1)
    for n in range(nout - 1):
        z1c += relay1(n, 0) + relay1(n, 1)
        z2c[2 * n].wait_recv()
        z2c[2 * n + 1].wait_recv()
        g2_o[...] += r2[n].astype(F32)
    relay1(nout - 1, 0)
    relay1(nout - 1, 1)
    for c in ld_copies:
        c.wait()
    loss_o[...] = functools.reduce(
        lambda a, b: a + b, [ldp[lax.rem(dp - g + ndp, ndp)] for g in range(ndp)]
    )
    for n in range(nout - 1):
        z1c[2 * n].wait_recv()
        z1c[2 * n + 1].wait_recv()
        g1_o[...] += r1[n].astype(F32)
    started = list(h_direct.values()) + list(h_passed.values()) + list(y2c.values())
    for c in started + list(y1c.values()) + u_copies + z2c + z1c:
        c.wait_send()


def shards(ndp, nsec, real_in, fake_in, kernel_first, kernel_second):
    cols, frames_in, cin = real_in.shape
    frames = frames_in // 3
    taps, whole, width = kernel_second.shape
    normaliser = float(cols * frames)
    count_all = float(cols * ndp * frames * whole)
    half = cols * frames
    rows = 2 * half
    c1, c2 = cin // ndp, whole // ndp
    nout = ndp // 2
    dma = pltpu.SemaphoreType.DMA
    loss, g1, g2 = pl.pallas_call(
        functools.partial(kernel, ndp, nsec, frames, normaliser),
        out_shape=(
            jax.ShapeDtypeStruct((8, 128), F32),
            jax.ShapeDtypeStruct((taps, c1, width), F32),
            jax.ShapeDtypeStruct((taps, c2, width), F32),
        ),
        in_specs=[pl.BlockSpec(memory_space=pl.ANY)] * 4,
        out_specs=(pl.BlockSpec(memory_space=pltpu.VMEM),) * 3,
        scratch_shapes=[
            pltpu.VMEM((2, 3 * half, cin), BF16),
            pltpu.VMEM((2 * cin // 128, 3 * half, 128), F32),
            pltpu.VMEM((rows, 3 * cin), BF16),
            pltpu.VMEM((taps * cin, width), BF16),
            pltpu.VMEM((taps, whole, width), BF16),
            pltpu.VMEM((nsec, rows, width), BF16),
            pltpu.VMEM((rows, width), F32),
            pltpu.VMEM((rows, width), F32),
            pltpu.VMEM((taps, rows, width), BF16),
            pltpu.VMEM((nsec - 1, rows, width), BF16),
            pltpu.VMEM((nsec - 1, rows, width), BF16),
            pltpu.VMEM((rows, width), F32),
            pltpu.VMEM((taps, whole, width), BF16),
            pltpu.VMEM((taps, cin, width), BF16),
            pltpu.VMEM((nout, taps, c2, width), BF16),
            pltpu.VMEM((nout, taps, c1, width), BF16),
            pltpu.VMEM((nout, taps, c2, width), BF16),
            pltpu.VMEM((nout, taps, c1, width), BF16),
            pltpu.VMEM((nout, taps, c2, width), BF16),
            pltpu.VMEM((nout, taps, c1, width), BF16),
            pltpu.VMEM((nsec, 8, 128), F32),
            pltpu.VMEM((ndp, 8, 128), F32),
            dma((4,)),
            dma((nsec, 2)), dma((nsec, 2)),
            dma((nsec - 1,)), dma((nsec - 1,)),
            dma((nout, 2)), dma((nout, 2)), dma((nout, 2)), dma((nout, 2)),
            dma((nout, 2)), dma((nout, 2)), dma((nout, 2)), dma((nout, 2)),
            dma((nsec - 1,)), dma((nsec - 1,)),
            dma((ndp - 1,)), dma((ndp - 1,)),
        ],
        compiler_params=pltpu.CompilerParams(collective_id=0, has_side_effects=True),
    )(
        real_in.reshape(3 * half, cin),
        fake_in.reshape(3 * half, cin),
        kernel_first.reshape(taps * cin, width),
        kernel_second,
    )
    return loss[:2, 0] / count_all, g1.transpose(1, 0, 2), g2.transpose(1, 0, 2)


def solution(mesh):
    return jax.shard_map(
        functools.partial(shards, mesh.shape["dp"], mesh.shape["section"]),
        mesh=mesh,
        in_specs=(
            P("dp", None, None),
            P("dp", None, None),
            P(None, None, "section"),
            P(None, None, "section"),
        ),
        out_specs=(P(), P("dp", None, "section"), P("dp", None, "section")),
        check_vma=False,
    )
```
